256 devices in a mesh: fsdp: 32 (over z, y), tp: 4 (over x), job: 2 (over core).
Axes of the slice: x: 4, y: 4, z: 8, core: 2. Of those that a mesh axis runs over, the one named last changes fastest.
Arguments:
- slopes_in: float32 [1024, 128, 1024], P('job', 'fsdp', 'tp'), parts along dimension 0, may hold values from -6 to 6
- moments_in: float32 [1024, 128, 1024], P('job', 'fsdp', 'tp'), parts along dimension 0, may hold values from -6 to 6
- weights_in: float32 [1024, 128, 1024], P('job', 'fsdp', 'tp'), parts along dimension 0, may hold values from -0.1875 to 0.1875
Outputs:
- new_weights: float32 [1024, 128, 1024], P('job', 'fsdp', 'tp'), parts along dimension 0
- new_momentum: float32 [1024, 128, 1024], P('job', 'fsdp', 'tp'), parts along dimension 0
The draws below stay inside these ranges and needn't reach their ends.
There are 2 independent parts, one for each index of `job`. The reference program is written for one: setup_inputs(seed, part) draws one part's arguments, and reference() takes and returns one part's arrays. A program takes and returns all parts, laid end to end along the dimension named above; each array names one. Nothing has to cross between parts.
All inputs are finite; a program needn't handle non-finite values.
Results may differ from the reference program's by a relative error of at most 0.00019.
Values sent between devices are 32-bit elements; how exact they have to be, the bound alone decides.
No kernel may reach another device: no remote copies, remote signals or barrier semaphores. Data moves between devices by JAX's collectives and lax.ppermute only.
A program may use at most 128 MiB of HBM per device.

```python
import jax
import jax.numpy as jnp
from jax import lax

SIDE = 128
WIDE = 1024
MATS = 512
ITERS = 5


def steps_of(stream_key, dims, shards, smallest, largest):
    def one(dim, parts):
        heights = jax.random.uniform(jax.random.fold_in(jax.random.fold_in(stream_key, 6), dim), (parts,), jnp.float32, smallest / len(shards), largest / len(shards))
        return jnp.repeat(jnp.exp(heights), dims[dim] // parts).reshape((-1,) + (1,) * (len(dims) - dim - 1))

    factor_of = one(*shards[0])
    for cut in shards[1:]:
        factor_of = factor_of * one(*cut)
    return factor_of


def scatter_about(own_key, extent, scale, bound, pieces=(), kind=jnp.bfloat16):
    drawn = jax.random.normal(own_key, extent, jnp.float32) * scale
    if len(pieces) > 0:
        drawn = steps_of(own_key, extent, pieces, -0.22, 0.18) * drawn
    return jnp.clip(drawn, min=-bound, max=bound).astype(kind)


def setup_inputs(seed: int = 0, part: int = 0) -> dict:
    arg_keys = jax.random.split(jax.random.key(seed), 4)
    part_splits = jax.random.split(jax.random.fold_in(arg_keys[3], part), 4)
    return {
        "slopes_in": scatter_about(part_splits[0], (MATS, SIDE, WIDE), 1.0, 6.0, ((1, 32), (2, 4)), jnp.float32),
        "moments_in": scatter_about(part_splits[1], (MATS, SIDE, WIDE), 1.0, 6.0, ((1, 32), (2, 4)), jnp.float32),
        "weights_in": scatter_about(part_splits[2], (MATS, SIDE, WIDE), 0.03, 0.1875, ((1, 32), (2, 4)), jnp.float32),
    }


hold_rate = 0.9
learn_rate = 0.8

def reference(slopes_in, moments_in, weights_in):
    new_momentum = hold_rate * moments_in + slopes_in

    def orthogonal_one(stack):
        iterate = stack[None]
        iterate = iterate * lax.rsqrt(lax.optimization_barrier(jnp.sum(iterate * iterate, axis=(1, 2), keepdims=True)) + 1e-06)
        for step in range(ITERS):
            gram = jnp.einsum('mik,mjk->mij', iterate, iterate, precision=lax.Precision.HIGHEST)
            mixed = -4.775 * gram + 2.0315 * jnp.einsum('mij,mjk->mik', gram, gram, precision=lax.Precision.HIGHEST)
            iterate = 3.4445 * iterate + jnp.einsum('mij,mjk->mik', mixed, iterate, precision=lax.Precision.HIGHEST)
        return iterate[0]
    iterate = lax.map(orthogonal_one, new_momentum)
    new_weights = weights_in - learn_rate * iterate
    return (new_weights, new_momentum)
```

```python
import jax
import jax.numpy as jnp
from jax import lax
from jax.sharding import PartitionSpec as P

ITERS = 5

hold_rate = 0.9
learn_rate = 0.8


def body(slopes_in, moments_in, weights_in):
    new_momentum = hold_rate * moments_in + slopes_in
    rows_axis = lax.axis_size("fsdp")
    cols_axis = lax.axis_size("tp")
    mats, rows, cols = new_momentum.shape
    own = mats // (rows_axis * cols_axis)
    moved = lax.all_to_all(
        new_momentum.reshape(rows_axis * cols_axis, own, rows, cols), ("fsdp", "tp"), 0, 0, tiled=True
    )
    iterate = moved.reshape(rows_axis, cols_axis, own, rows, cols).transpose(2, 0, 3, 1, 4)
    iterate = iterate.reshape(own, rows_axis * rows, cols_axis * cols)
    iterate = iterate * lax.rsqrt(jnp.sum(iterate * iterate, axis=(1, 2), keepdims=True) + 1e-06)
    for step in range(ITERS):
        gram = jnp.einsum("mik,mjk->mij", iterate, iterate, precision=lax.Precision.HIGHEST)
        mixed = -4.775 * gram + 2.0315 * jnp.einsum(
            "mij,mjk->mik", gram, gram, precision=lax.Precision.HIGHEST
        )
        iterate = 3.4445 * iterate + jnp.einsum(
            "mij,mjk->mik", mixed, iterate, precision=lax.Precision.HIGHEST
        )
    back = iterate.reshape(own, rows_axis, rows, cols_axis, cols).transpose(1, 3, 0, 2, 4)
    back = lax.all_to_all(
        back.reshape(rows_axis * cols_axis, own, rows, cols), ("fsdp", "tp"), 0, 0, tiled=True
    )
    new_weights = weights_in - learn_rate * back.reshape(mats, rows, cols)
    return (new_weights, new_momentum)


def solution(mesh):
    placed = P("job", "fsdp", "tp")
    return jax.shard_map(
        body, mesh=mesh, in_specs=(placed,) * 3, out_specs=(placed,) * 2, check_vma=False
    )
```

```python
import jax
import jax.numpy as jnp
from jax import lax
from jax.experimental import pallas as pl
from jax.experimental.pallas import tpu as pltpu
from jax.sharding import PartitionSpec as P

ITERS = 5
WINDOWS = (2, 3)

hold_rate = 0.9
learn_rate = 0.8

ROWS_BY_ROWS = (((1,), (1,)), ((), ()))
ROWS_BY_COLS = (((1,), (0,)), ((), ()))


def product(left, right, dims=ROWS_BY_COLS):
    return lax.dot_general(
        left, right, dims, precision=lax.Precision.HIGHEST, preferred_element_type=jnp.float32
    )


def orthogonalize(stack):
    side = stack[0].shape[0]
    unit = lax.broadcasted_iota(jnp.int32, (side, side), 0) == lax.broadcasted_iota(
        jnp.int32, (side, side), 1
    )
    scaled_unit = 3.4445 * unit.astype(jnp.float32)
    stack = [x * lax.rsqrt(jnp.sum(x * x, keepdims=True) + 1e-06) for x in stack]
    assert sum(WINDOWS) == ITERS
    for window in WINDOWS:
        grams = [product(x, x, ROWS_BY_ROWS) for x in stack]
        total = None
        for step in range(window):
            mixed = [scaled_unit + (-4.775 * a + 2.0315 * product(a, a)) for a in grams]
            total = mixed if total is None else [product(m, t) for m, t in zip(mixed, total)]
            if step < window - 1:
                grams = [product(product(m, a), m) for m, a in zip(mixed, grams)]
        stack = [product(t, x) for t, x in zip(total, stack)]
    return stack


def kernel(moved, back, whole):
    groups, cuts, own, rows, cols = moved.shape

    def gather(pair, carry):
        for m in range(own):
            for x in range(cuts):
                columns = slice(x * cols, (x + 1) * cols)
                whole[m, pair, 0:rows, columns] = moved[2 * pair, x, m]
                whole[m, pair, rows : 2 * rows, columns] = moved[2 * pair + 1, x, m]
        return carry

    def scatter(pair, carry):
        for m in range(own):
            for x in range(cuts):
                columns = slice(x * cols, (x + 1) * cols)
                back[2 * pair, x, m] = whole[m, pair, 0:rows, columns]
                back[2 * pair + 1, x, m] = whole[m, pair, rows : 2 * rows, columns]
        return carry

    lax.fori_loop(0, groups // 2, gather, 0, unroll=2)
    stack = orthogonalize([whole[m].reshape(groups * rows, cuts * cols) for m in range(own)])
    for m in range(own):
        whole[m] = (learn_rate * stack[m]).reshape(groups // 2, 2 * rows, cuts * cols)
    lax.fori_loop(0, groups // 2, scatter, 0, unroll=2)


def steps_of(moved):
    groups, cuts, own, rows, cols = moved.shape
    return pl.pallas_call(
        kernel,
        out_shape=jax.ShapeDtypeStruct(moved.shape, moved.dtype),
        in_specs=[pl.BlockSpec(memory_space=pltpu.VMEM)],
        out_specs=pl.BlockSpec(memory_space=pltpu.VMEM),
        scratch_shapes=[pltpu.VMEM((own, groups // 2, 2 * rows, cuts * cols), jnp.float32)],
        compiler_params=pltpu.CompilerParams(vmem_limit_bytes=32 * 2**20),
        name="steps",
    )(moved)


def body(slopes_in, moments_in, weights_in):
    new_momentum = hold_rate * moments_in + slopes_in
    groups = lax.axis_size("fsdp")
    cuts = lax.axis_size("tp")
    mats, rows, cols = new_momentum.shape
    own = mats // (groups * cuts)
    moved = lax.all_to_all(
        new_momentum.reshape(groups * cuts, own, rows, cols), ("fsdp", "tp"), 0, 0, tiled=True
    )
    back = steps_of(moved.reshape(groups, cuts, own, rows, cols))
    back = lax.all_to_all(
        back.reshape(groups * cuts, own, rows, cols), ("fsdp", "tp"), 0, 0, tiled=True
    )
    new_weights = weights_in - back.reshape(mats, rows, cols)
    return (new_weights, new_momentum)


def solution(mesh):
    placed = P("job", "fsdp", "tp")
    return jax.shard_map(
        body, mesh=mesh, in_specs=(placed,) * 3, out_specs=(placed,) * 2, check_vma=False
    )
```

```python
import jax
import jax.numpy as jnp
from jax import lax
from jax.experimental import pallas as pl
from jax.experimental.pallas import tpu as pltpu
from jax.sharding import PartitionSpec as P

ITERS = 5
WINDOWS = (2, 3)

hold_rate = 0.9
learn_rate = 0.8

TURN_NS = 25000

ROWS_BY_ROWS = (((1,), (1,)), ((), ()))
ROWS_BY_COLS = (((1,), (0,)), ((), ()))


def product(left, right):
    return lax.dot_general(
        left,
        right,
        ROWS_BY_COLS,
        precision=lax.Precision.HIGHEST,
        preferred_element_type=jnp.float32,
    )


def split(x):
    high = x.astype(jnp.bfloat16)
    rest = x - high.astype(jnp.float32)
    middle = rest.astype(jnp.bfloat16)
    low = (rest - middle.astype(jnp.float32)).astype(jnp.bfloat16)
    return high, middle, low


def term(left, right, dims=ROWS_BY_COLS):
    return lax.dot_general(left, right, dims, preferred_element_type=jnp.float32)


def gram_of(x):
    high, middle, low = split(x)
    mixed = term(high, middle, ROWS_BY_ROWS) + term(high, low, ROWS_BY_ROWS)
    small = mixed + mixed.T + term(middle, middle, ROWS_BY_ROWS)
    return term(high, high, ROWS_BY_ROWS) + small


def applied(left, right):
    lh, lm, ll = split(left)
    rh, rm, rl = split(right)
    pair = term(jnp.concatenate((lh, lm), 1), jnp.concatenate((rm, rh), 0))
    small = term(jnp.concatenate((lh, ll), 1), jnp.concatenate((rl, rh), 0)) + term(lm, rm)
    return term(lh, rh) + (pair + small)


def orthogonalize(stack):
    side = stack[0].shape[0]
    unit = lax.broadcasted_iota(jnp.int32, (side, side), 0) == lax.broadcasted_iota(
        jnp.int32, (side, side), 1
    )
    scaled_unit = 3.4445 * unit.astype(jnp.float32)
    stack = [x * lax.rsqrt(jnp.sum(x * x, keepdims=True) + 1e-06) for x in stack]
    assert sum(WINDOWS) == ITERS
    for window in WINDOWS:
        grams = [gram_of(x) for x in stack]
        total = None
        for step in range(window):
            mixed = [scaled_unit + (-4.775 * a + 2.0315 * product(a, a)) for a in grams]
            total = mixed if total is None else [product(m, t) for m, t in zip(mixed, total)]
            if step < window - 1:
                grams = [product(product(m, a), m) for m, a in zip(mixed, grams)]
        stack = [applied(t, x) for t, x in zip(total, stack)]
    return stack


def kernel(moved, back, whole):
    groups, cuts, own, rows, cols = moved.shape

    def gather(pair, carry):
        for m in range(own):
            for x in range(cuts):
                columns = slice(x * cols, (x + 1) * cols)
                whole[m, pair, 0:rows, columns] = moved[2 * pair, x, m]
                whole[m, pair, rows : 2 * rows, columns] = moved[2 * pair + 1, x, m]
        return carry

    def scatter(pair, carry):
        for m in range(own):
            for x in range(cuts):
                columns = slice(x * cols, (x + 1) * cols)
                back[2 * pair, x, m] = whole[m, pair, 0:rows, columns]
                back[2 * pair + 1, x, m] = whole[m, pair, rows : 2 * rows, columns]
        return carry

    lax.fori_loop(0, groups // 2, gather, 0, unroll=2)
    stack = orthogonalize([whole[m].reshape(groups * rows, cuts * cols) for m in range(own)])
    for m in range(own):
        whole[m] = (learn_rate * stack[m]).reshape(groups // 2, 2 * rows, cuts * cols)
    lax.fori_loop(0, groups // 2, scatter, 0, unroll=2)


def steps_of(moved):
    groups, cuts, own, rows, cols = moved.shape
    return pl.pallas_call(
        kernel,
        out_shape=jax.ShapeDtypeStruct(moved.shape, moved.dtype),
        in_specs=[pl.BlockSpec(memory_space=pltpu.VMEM)],
        out_specs=pl.BlockSpec(memory_space=pltpu.VMEM),
        scratch_shapes=[pltpu.VMEM((own, groups // 2, 2 * rows, cuts * cols), jnp.float32)],
        compiler_params=pltpu.CompilerParams(vmem_limit_bytes=32 * 2**20),
        name="steps",
    )(moved)


def momentum_kernel(slopes_hbm, moments_hbm, momentum, slopes, moments, arrived):
    chunks = arrived.shape[1]
    per = slopes.shape[0] // chunks
    copies = []
    for c in range(chunks):
        part = pl.ds(c * per, per)
        copies.append(
            (
                pltpu.make_async_copy(slopes_hbm.at[part], slopes.at[part], arrived.at[0, c]),
                pltpu.make_async_copy(moments_hbm.at[part], moments.at[part], arrived.at[1, c]),
            )
        )
        for copy in copies[-1]:
            copy.start()
    for c in range(chunks):
        for copy in copies[c]:
            copy.wait()

        def some(i, carry):
            part = pl.ds(c * per + i * 16, 16)
            momentum[part] = hold_rate * moments[part] + slopes[part]
            return carry

        lax.fori_loop(0, per // 16, some, 0)

    @pl.when(lax.axis_index("job") == 1)
    def _():
        pl.delay(TURN_NS)


def momentum_of(slopes_in, moments_in):
    hbm = [pltpu.with_memory_space_constraint(x, pltpu.HBM) for x in (slopes_in, moments_in)]
    return pl.pallas_call(
        momentum_kernel,
        out_shape=jax.ShapeDtypeStruct(slopes_in.shape, slopes_in.dtype),
        in_specs=[pl.BlockSpec(memory_space=pltpu.HBM)] * 2,
        out_specs=pl.BlockSpec(memory_space=pltpu.VMEM),
        scratch_shapes=[
            pltpu.VMEM(slopes_in.shape, jnp.float32),
            pltpu.VMEM(slopes_in.shape, jnp.float32),
            pltpu.SemaphoreType.DMA((2, 4)),
        ],
        compiler_params=pltpu.CompilerParams(vmem_limit_bytes=16 * 2**20),
        name="momentum",
    )(*hbm)


def body(slopes_in, moments_in, weights_in):
    new_momentum = momentum_of(slopes_in, moments_in)
    groups = lax.axis_size("fsdp")
    cuts = lax.axis_size("tp")
    mats, rows, cols = new_momentum.shape
    own = mats // (groups * cuts)
    moved = lax.all_to_all(
        new_momentum.reshape(groups * cuts, own, rows, cols), ("fsdp", "tp"), 0, 0, tiled=True
    )
    back = steps_of(moved.reshape(groups, cuts, own, rows, cols))
    back = lax.all_to_all(
        back.reshape(groups * cuts, own, rows, cols), ("fsdp", "tp"), 0, 0, tiled=True
    )
    new_weights = weights_in - back.reshape(mats, rows, cols)
    return (new_weights, new_momentum)


def solution(mesh):
    placed = P("job", "fsdp", "tp")
    return jax.shard_map(
        body, mesh=mesh, in_specs=(placed,) * 3, out_specs=(placed,) * 2, check_vma=False
    )
```

```python
import jax
import jax.numpy as jnp
from jax import lax
from jax.experimental import pallas as pl
from jax.experimental.pallas import tpu as pltpu
from jax.sharding import PartitionSpec as P

ITERS = 5
WINDOWS = (2, 3)

hold_rate = 0.9
learn_rate = 0.8

TURN_NS = 25000

CHUNKS = 4
BLOCK = 16

ROWS_BY_ROWS = (((1,), (1,)), ((), ()))
ROWS_BY_COLS = (((1,), (0,)), ((), ()))


def product(left, right):
    return lax.dot_general(
        left,
        right,
        ROWS_BY_COLS,
        precision=lax.Precision.HIGHEST,
        preferred_element_type=jnp.float32,
    )


def split(x):
    high = x.astype(jnp.bfloat16)
    rest = x - high.astype(jnp.float32)
    middle = rest.astype(jnp.bfloat16)
    low = (rest - middle.astype(jnp.float32)).astype(jnp.bfloat16)
    return high, middle, low


def term(left, right, dims=ROWS_BY_COLS):
    return lax.dot_general(left, right, dims, preferred_element_type=jnp.float32)


def gram_of(x):
    high, middle, low = split(x)
    mixed = term(high, middle, ROWS_BY_ROWS) + term(high, low, ROWS_BY_ROWS)
    small = mixed + mixed.T + term(middle, middle, ROWS_BY_ROWS)
    return term(high, high, ROWS_BY_ROWS) + small


def applied(left, right):
    lh, lm, ll = split(left)
    rh, rm, rl = split(right)
    pair = term(jnp.concatenate((lh, lm), 1), jnp.concatenate((rm, rh), 0))
    small = term(jnp.concatenate((lh, ll), 1), jnp.concatenate((rl, rh), 0)) + term(lm, rm)
    return term(lh, rh) + (pair + small)


def orthogonalize(stack):
    side = stack[0].shape[0]
    unit = lax.broadcasted_iota(jnp.int32, (side, side), 0) == lax.broadcasted_iota(
        jnp.int32, (side, side), 1
    )
    scaled_unit = 3.4445 * unit.astype(jnp.float32)
    stack = [x * lax.rsqrt(jnp.sum(x * x, keepdims=True) + 1e-06) for x in stack]
    assert sum(WINDOWS) == ITERS
    for window in WINDOWS:
        grams = [gram_of(x) for x in stack]
        total = None
        for step in range(window):
            mixed = [scaled_unit + (-4.775 * a + 2.0315 * product(a, a)) for a in grams]
            total = mixed if total is None else [product(m, t) for m, t in zip(mixed, total)]
            if step < window - 1:
                grams = [product(product(m, a), m) for m, a in zip(mixed, grams)]
        stack = [applied(t, x) for t, x in zip(total, stack)]
    return stack


def kernel(moved, back, whole):
    groups, cuts, own, rows, cols = moved.shape

    def gather(pair, carry):
        for m in range(own):
            for x in range(cuts):
                columns = slice(x * cols, (x + 1) * cols)
                whole[m, pair, 0:rows, columns] = moved[2 * pair, x, m]
                whole[m, pair, rows : 2 * rows, columns] = moved[2 * pair + 1, x, m]
        return carry

    def scatter(pair, carry):
        for m in range(own):
            for x in range(cuts):
                columns = slice(x * cols, (x + 1) * cols)
                back[2 * pair, x, m] = whole[m, pair, 0:rows, columns]
                back[2 * pair + 1, x, m] = whole[m, pair, rows : 2 * rows, columns]
        return carry

    lax.fori_loop(0, groups // 2, gather, 0, unroll=2)
    stack = orthogonalize([whole[m].reshape(groups * rows, cuts * cols) for m in range(own)])
    for m in range(own):
        whole[m] = (learn_rate * stack[m]).reshape(groups // 2, 2 * rows, cuts * cols)
    lax.fori_loop(0, groups // 2, scatter, 0, unroll=2)


def steps_of(moved):
    groups, cuts, own, rows, cols = moved.shape
    return pl.pallas_call(
        kernel,
        out_shape=jax.ShapeDtypeStruct(moved.shape, moved.dtype),
        in_specs=[pl.BlockSpec(memory_space=pltpu.VMEM)],
        out_specs=pl.BlockSpec(memory_space=pltpu.VMEM),
        scratch_shapes=[pltpu.VMEM((own, groups // 2, 2 * rows, cuts * cols), jnp.float32)],
        compiler_params=pltpu.CompilerParams(vmem_limit_bytes=32 * 2**20),
        name="steps",
    )(moved)


def momentum_kernel(slopes_hbm, moments_hbm, momentum_hbm, slopes, moments, arrived, stored):
    chunks = arrived.shape[1]
    per = slopes.shape[0] // chunks
    parts = [pl.ds(c * per, per) for c in range(chunks)]
    loads = [
        (
            pltpu.make_async_copy(slopes_hbm.at[part], slopes.at[part], arrived.at[0, c]),
            pltpu.make_async_copy(moments_hbm.at[part], moments.at[part], arrived.at[1, c]),
        )
        for c, part in enumerate(parts)
    ]
    stores = [
        pltpu.make_async_copy(slopes.at[part], momentum_hbm.at[part], stored.at[c])
        for c, part in enumerate(parts)
    ]
    for pair in loads:
        for copy in pair:
            copy.start()
    for c in range(chunks):
        for copy in loads[c]:
            copy.wait()

        def some(i, carry):
            part = pl.ds(c * per + i * BLOCK, BLOCK)
            slopes[part] = hold_rate * moments[part] + slopes[part]
            return carry

        lax.fori_loop(0, per // BLOCK, some, 0)
        stores[c].start()

    @pl.when(lax.axis_index("job") == 1)
    def _():
        pl.delay(TURN_NS)

    for copy in stores:
        copy.wait()


def momentum_of(slopes_in, moments_in):
    hbm = [pltpu.with_memory_space_constraint(x, pltpu.HBM) for x in (slopes_in, moments_in)]
    return pl.pallas_call(
        momentum_kernel,
        out_shape=jax.ShapeDtypeStruct(slopes_in.shape, slopes_in.dtype),
        in_specs=[pl.BlockSpec(memory_space=pltpu.HBM)] * 2,
        out_specs=pl.BlockSpec(memory_space=pltpu.HBM),
        scratch_shapes=[
            pltpu.VMEM(slopes_in.shape, jnp.float32),
            pltpu.VMEM(slopes_in.shape, jnp.float32),
            pltpu.SemaphoreType.DMA((2, CHUNKS)),
            pltpu.SemaphoreType.DMA((CHUNKS,)),
        ],
        compiler_params=pltpu.CompilerParams(vmem_limit_bytes=16 * 2**20),
        name="momentum",
    )(*hbm)


def weights_kernel(weights, back, new_hbm, new, stored):
    chunks = stored.shape[0]
    per = new.shape[0] // chunks
    stores = []
    for c in range(chunks):

        def some(i, carry):
            part = pl.ds(c * per + i * BLOCK, BLOCK)
            new[part] = weights[part] - back[part]
            return carry

        lax.fori_loop(0, per // BLOCK, some, 0)
        part = pl.ds(c * per, per)
        stores.append(pltpu.make_async_copy(new.at[part], new_hbm.at[part], stored.at[c]))
        stores[-1].start()
    for copy in stores:
        copy.wait()


def weights_of(weights_in, back):
    return pl.pallas_call(
        weights_kernel,
        out_shape=jax.ShapeDtypeStruct(weights_in.shape, weights_in.dtype),
        in_specs=[pl.BlockSpec(memory_space=pltpu.VMEM)] * 2,
        out_specs=pl.BlockSpec(memory_space=pltpu.HBM),
        scratch_shapes=[
            pltpu.VMEM(weights_in.shape, jnp.float32),
            pltpu.SemaphoreType.DMA((CHUNKS,)),
        ],
        compiler_params=pltpu.CompilerParams(vmem_limit_bytes=16 * 2**20),
        name="new_weights",
    )(weights_in, back)


def body(slopes_in, moments_in, weights_in):
    new_momentum = momentum_of(slopes_in, moments_in)
    groups = lax.axis_size("fsdp")
    cuts = lax.axis_size("tp")
    mats, rows, cols = new_momentum.shape
    own = mats // (groups * cuts)
    moved = lax.all_to_all(
        new_momentum.reshape(groups * cuts, own, rows, cols), ("fsdp", "tp"), 0, 0, tiled=True
    )
    back = steps_of(moved.reshape(groups, cuts, own, rows, cols))
    back = lax.all_to_all(
        back.reshape(groups * cuts, own, rows, cols), ("fsdp", "tp"), 0, 0, tiled=True
    )
    new_weights = weights_of(weights_in, back.reshape(mats, rows, cols))
    return (new_weights, new_momentum)


def solution(mesh):
    placed = P("job", "fsdp", "tp")
    return jax.shard_map(
        body, mesh=mesh, in_specs=(placed,) * 3, out_specs=(placed,) * 2, check_vma=False
    )
```

```python
import jax
import jax.numpy as jnp
from jax import lax
from jax.experimental import pallas as pl
from jax.experimental.pallas import tpu as pltpu
from jax.sharding import PartitionSpec as P

ITERS = 5
WINDOWS = (2, 3)

hold_rate = 0.9
learn_rate = 0.8

TURN_NS = 24500

CHUNKS = 4
BLOCK = 16

ROWS_BY_ROWS = (((1,), (1,)), ((), ()))
ROWS_BY_COLS = (((1,), (0,)), ((), ()))


def product(left, right):
    return lax.dot_general(
        left,
        right,
        ROWS_BY_COLS,
        precision=lax.Precision.HIGHEST,
        preferred_element_type=jnp.float32,
    )


def split(x):
    high = x.astype(jnp.bfloat16)
    rest = x - high.astype(jnp.float32)
    middle = rest.astype(jnp.bfloat16)
    low = (rest - middle.astype(jnp.float32)).astype(jnp.bfloat16)
    return high, middle, low


def term(left, right, dims=ROWS_BY_COLS):
    return lax.dot_general(left, right, dims, preferred_element_type=jnp.float32)


def gram_of(x):
    high, middle, low = split(x)
    mixed = term(high, middle, ROWS_BY_ROWS) + term(high, low, ROWS_BY_ROWS)
    small = mixed + mixed.T + term(middle, middle, ROWS_BY_ROWS)
    return term(high, high, ROWS_BY_ROWS) + small


def applied(left, right):
    lh, lm, ll = split(left)
    rh, rm, rl = split(right)
    pair = term(jnp.concatenate((lh, lm), 1), jnp.concatenate((rm, rh), 0))
    small = term(jnp.concatenate((lh, ll), 1), jnp.concatenate((rl, rh), 0)) + term(lm, rm)
    return term(lh, rh) + (pair + small)


def orthogonalize(stack):
    side = stack[0].shape[0]
    unit = lax.broadcasted_iota(jnp.int32, (side, side), 0) == lax.broadcasted_iota(
        jnp.int32, (side, side), 1
    )
    scaled_unit = 3.4445 * unit.astype(jnp.float32)
    stack = [x * lax.rsqrt(jnp.sum(x * x, keepdims=True) + 1e-06) for x in stack]
    assert sum(WINDOWS) == ITERS
    for window in WINDOWS:
        grams = [gram_of(x) for x in stack]
        total = None
        for step in range(window):
            mixed = [scaled_unit + (-4.775 * a + 2.0315 * product(a, a)) for a in grams]
            total = mixed if total is None else [product(m, t) for m, t in zip(mixed, total)]
            if step < window - 1:
                grams = [product(product(m, a), m) for m, a in zip(mixed, grams)]
        stack = [applied(t, x) for t, x in zip(total, stack)]
    return stack


def kernel(moved, momentum, back, momentum_hbm, whole, stored):
    groups, cuts, own, rows, cols = moved.shape
    store = pltpu.make_async_copy(momentum, momentum_hbm, stored)
    store.start()

    def gather(pair, carry):
        for m in range(own):
            for x in range(cuts):
                columns = slice(x * cols, (x + 1) * cols)
                whole[m, pair, 0:rows, columns] = moved[2 * pair, x, m]
                whole[m, pair, rows : 2 * rows, columns] = moved[2 * pair + 1, x, m]
        return carry

    def scatter(pair, carry):
        for m in range(own):
            for x in range(cuts):
                columns = slice(x * cols, (x + 1) * cols)
                back[2 * pair, x, m] = whole[m, pair, 0:rows, columns]
                back[2 * pair + 1, x, m] = whole[m, pair, rows : 2 * rows, columns]
        return carry

    lax.fori_loop(0, groups // 2, gather, 0, unroll=2)
    stack = orthogonalize([whole[m].reshape(groups * rows, cuts * cols) for m in range(own)])
    for m in range(own):
        whole[m] = (learn_rate * stack[m]).reshape(groups // 2, 2 * rows, cuts * cols)
    lax.fori_loop(0, groups // 2, scatter, 0, unroll=2)
    store.wait()


def steps_of(moved, momentum):
    groups, cuts, own, rows, cols = moved.shape
    return pl.pallas_call(
        kernel,
        out_shape=(
            jax.ShapeDtypeStruct(moved.shape, moved.dtype),
            jax.ShapeDtypeStruct(momentum.shape, momentum.dtype),
        ),
        in_specs=[pl.BlockSpec(memory_space=pltpu.VMEM)] * 2,
        out_specs=(
            pl.BlockSpec(memory_space=pltpu.VMEM),
            pl.BlockSpec(memory_space=pltpu.HBM),
        ),
        scratch_shapes=[
            pltpu.VMEM((own, groups // 2, 2 * rows, cuts * cols), jnp.float32),
            pltpu.SemaphoreType.DMA(()),
        ],
        compiler_params=pltpu.CompilerParams(vmem_limit_bytes=32 * 2**20),
        name="steps",
    )(moved, momentum)


def momentum_kernel(slopes_hbm, moments_hbm, momentum, slopes, moments, arrived):
    chunks = arrived.shape[1]
    per = slopes.shape[0] // chunks
    parts = [pl.ds(c * per, per) for c in range(chunks)]
    loads = [
        (
            pltpu.make_async_copy(slopes_hbm.at[part], slopes.at[part], arrived.at[0, c]),
            pltpu.make_async_copy(moments_hbm.at[part], moments.at[part], arrived.at[1, c]),
        )
        for c, part in enumerate(parts)
    ]
    for pair in loads:
        for copy in pair:
            copy.start()
    for c in range(chunks):
        for copy in loads[c]:
            copy.wait()

        def some(i, carry):
            part = pl.ds(c * per + i * BLOCK, BLOCK)
            momentum[part] = hold_rate * moments[part] + slopes[part]
            return carry

        lax.fori_loop(0, per // BLOCK, some, 0)

    @pl.when(lax.axis_index("job") == 1)
    def _():
        pl.delay(TURN_NS)


def momentum_of(slopes_in, moments_in):
    hbm = [pltpu.with_memory_space_constraint(x, pltpu.HBM) for x in (slopes_in, moments_in)]
    return pl.pallas_call(
        momentum_kernel,
        out_shape=pltpu.VMEM(slopes_in.shape, slopes_in.dtype),
        in_specs=[pl.BlockSpec(memory_space=pltpu.HBM)] * 2,
        out_specs=pl.BlockSpec(memory_space=pltpu.VMEM),
        scratch_shapes=[
            pltpu.VMEM(slopes_in.shape, jnp.float32),
            pltpu.VMEM(slopes_in.shape, jnp.float32),
            pltpu.SemaphoreType.DMA((2, CHUNKS)),
        ],
        compiler_params=pltpu.CompilerParams(vmem_limit_bytes=16 * 2**20),
        name="momentum",
    )(*hbm)


def weights_kernel(weights, back, new_hbm, new, stored):
    chunks = stored.shape[0]
    per = new.shape[0] // chunks
    stores = []
    for c in range(chunks):

        def some(i, carry):
            part = pl.ds(c * per + i * BLOCK, BLOCK)
            new[part] = weights[part] - back[part]
            return carry

        lax.fori_loop(0, per // BLOCK, some, 0)
        part = pl.ds(c * per, per)
        stores.append(pltpu.make_async_copy(new.at[part], new_hbm.at[part], stored.at[c]))
        stores[-1].start()
    for copy in stores:
        copy.wait()


def weights_of(weights_in, back):
    return pl.pallas_call(
        weights_kernel,
        out_shape=jax.ShapeDtypeStruct(weights_in.shape, weights_in.dtype),
        in_specs=[pl.BlockSpec(memory_space=pltpu.VMEM)] * 2,
        out_specs=pl.BlockSpec(memory_space=pltpu.HBM),
        scratch_shapes=[
            pltpu.VMEM(weights_in.shape, jnp.float32),
            pltpu.SemaphoreType.DMA((CHUNKS,)),
        ],
        compiler_params=pltpu.CompilerParams(vmem_limit_bytes=16 * 2**20),
        name="new_weights",
    )(weights_in, back)


def body(slopes_in, moments_in, weights_in):
    momentum = momentum_of(slopes_in, moments_in)
    groups = lax.axis_size("fsdp")
    cuts = lax.axis_size("tp")
    mats, rows, cols = momentum.shape
    own = mats // (groups * cuts)
    moved = lax.all_to_all(
        momentum.reshape(groups * cuts, own, rows, cols), ("fsdp", "tp"), 0, 0, tiled=True
    )
    back, new_momentum = steps_of(moved.reshape(groups, cuts, own, rows, cols), momentum)
    back = lax.all_to_all(
        back.reshape(groups * cuts, own, rows, cols), ("fsdp", "tp"), 0, 0, tiled=True
    )
    new_weights = weights_of(weights_in, back.reshape(mats, rows, cols))
    return (new_weights, new_momentum)


def solution(mesh):
    placed = P("job", "fsdp", "tp")
    return jax.shard_map(
        body, mesh=mesh, in_specs=(placed,) * 3, out_specs=(placed,) * 2, check_vma=False
    )
```

```python
import jax
import jax.numpy as jnp
from jax import lax
from jax.experimental import pallas as pl
from jax.experimental.pallas import tpu as pltpu
from jax.sharding import PartitionSpec as P

ITERS = 5
WINDOWS = (2, 3)

hold_rate = 0.9
learn_rate = 0.8

TURN_NS = 24500

CHUNKS = 4
BLOCK = 16

ROWS_BY_ROWS = (((1,), (1,)), ((), ()))
ROWS_BY_COLS = (((1,), (0,)), ((), ()))


def product(left, right):
    return lax.dot_general(
        left,
        right,
        ROWS_BY_COLS,
        precision=lax.Precision.HIGHEST,
        preferred_element_type=jnp.float32,
    )


def split(x):
    high = x.astype(jnp.bfloat16)
    rest = x - high.astype(jnp.float32)
    middle = rest.astype(jnp.bfloat16)
    low = (rest - middle.astype(jnp.float32)).astype(jnp.bfloat16)
    return high, middle, low


def term(left, right, dims=ROWS_BY_COLS):
    return lax.dot_general(left, right, dims, preferred_element_type=jnp.float32)


def gram_of(x):
    high, middle, low = split(x)
    mixed = term(high, middle, ROWS_BY_ROWS) + term(high, low, ROWS_BY_ROWS)
    small = mixed + mixed.T + term(middle, middle, ROWS_BY_ROWS)
    return term(high, high, ROWS_BY_ROWS) + small


def applied(left, right):
    lh, lm, ll = split(left)
    rh, rm, rl = split(right)
    pair = term(jnp.concatenate((lh, lm), 1), jnp.concatenate((rm, rh), 0))
    small = term(jnp.concatenate((lh, ll), 1), jnp.concatenate((rl, rh), 0)) + term(lm, rm)
    return term(lh, rh) + (pair + small)


def orthogonalize(stack):
    side = stack[0].shape[0]
    unit = lax.broadcasted_iota(jnp.int32, (side, side), 0) == lax.broadcasted_iota(
        jnp.int32, (side, side), 1
    )
    unit = unit.astype(jnp.float32)
    scaled_unit = 3.4445 * unit
    scales = None
    assert sum(WINDOWS) == ITERS
    for window in WINDOWS:
        grams = [gram_of(x) for x in stack]
        if scales is None:
            scales = [lax.rsqrt(jnp.sum(a * unit, keepdims=True) + 1e-06) for a in grams]
            grams = [(r * r) * a for r, a in zip(scales, grams)]
            factors = scales
        else:
            factors = [None] * len(stack)
        total = None
        for step in range(window):
            mixed = [scaled_unit + (-4.775 * a + 2.0315 * product(a, a)) for a in grams]
            total = mixed if total is None else [product(m, t) for m, t in zip(mixed, total)]
            if step < window - 1:
                grams = [product(product(m, a), m) for m, a in zip(mixed, grams)]
        total = [t if f is None else f * t for f, t in zip(factors, total)]
        stack = [applied(t, x) for t, x in zip(total, stack)]
    return stack


def kernel(moved, momentum, back, momentum_hbm, whole, stored):
    groups, cuts, own, rows, cols = moved.shape
    store = pltpu.make_async_copy(momentum, momentum_hbm, stored)
    store.start()

    def gather(pair, carry):
        for m in range(own):
            for x in range(cuts):
                columns = slice(x * cols, (x + 1) * cols)
                whole[m, pair, 0:rows, columns] = moved[2 * pair, x, m]
                whole[m, pair, rows : 2 * rows, columns] = moved[2 * pair + 1, x, m]
        return carry

    def scatter(pair, carry):
        for m in range(own):
            for x in range(cuts):
                columns = slice(x * cols, (x + 1) * cols)
                back[2 * pair, x, m] = whole[m, pair, 0:rows, columns]
                back[2 * pair + 1, x, m] = whole[m, pair, rows : 2 * rows, columns]
        return carry

    lax.fori_loop(0, groups // 2, gather, 0, unroll=2)
    stack = orthogonalize([whole[m].reshape(groups * rows, cuts * cols) for m in range(own)])
    for m in range(own):
        whole[m] = (learn_rate * stack[m]).reshape(groups // 2, 2 * rows, cuts * cols)
    lax.fori_loop(0, groups // 2, scatter, 0, unroll=2)
    store.wait()


def steps_of(moved, momentum):
    groups, cuts, own, rows, cols = moved.shape
    return pl.pallas_call(
        kernel,
        out_shape=(
            jax.ShapeDtypeStruct(moved.shape, moved.dtype),
            jax.ShapeDtypeStruct(momentum.shape, momentum.dtype),
        ),
        in_specs=[pl.BlockSpec(memory_space=pltpu.VMEM)] * 2,
        out_specs=(
            pl.BlockSpec(memory_space=pltpu.VMEM),
            pl.BlockSpec(memory_space=pltpu.HBM),
        ),
        scratch_shapes=[
            pltpu.VMEM((own, groups // 2, 2 * rows, cuts * cols), jnp.float32),
            pltpu.SemaphoreType.DMA(()),
        ],
        compiler_params=pltpu.CompilerParams(vmem_limit_bytes=32 * 2**20),
        name="steps",
    )(moved, momentum)


def momentum_kernel(slopes_hbm, moments_hbm, momentum, slopes, moments, arrived):
    chunks = arrived.shape[1]
    per = slopes.shape[0] // chunks
    parts = [pl.ds(c * per, per) for c in range(chunks)]
    loads = [
        (
            pltpu.make_async_copy(slopes_hbm.at[part], slopes.at[part], arrived.at[0, c]),
            pltpu.make_async_copy(moments_hbm.at[part], moments.at[part], arrived.at[1, c]),
        )
        for c, part in enumerate(parts)
    ]
    for pair in loads:
        for copy in pair:
            copy.start()
    for c in range(chunks):
        for copy in loads[c]:
            copy.wait()

        def some(i, carry):
            part = pl.ds(c * per + i * BLOCK, BLOCK)
            momentum[part] = hold_rate * moments[part] + slopes[part]
            return carry

        lax.fori_loop(0, per // BLOCK, some, 0)

    @pl.when(lax.axis_index("job") == 1)
    def _():
        pl.delay(TURN_NS)


def momentum_of(slopes_in, moments_in):
    hbm = [pltpu.with_memory_space_constraint(x, pltpu.HBM) for x in (slopes_in, moments_in)]
    return pl.pallas_call(
        momentum_kernel,
        out_shape=pltpu.VMEM(slopes_in.shape, slopes_in.dtype),
        in_specs=[pl.BlockSpec(memory_space=pltpu.HBM)] * 2,
        out_specs=pl.BlockSpec(memory_space=pltpu.VMEM),
        scratch_shapes=[
            pltpu.VMEM(slopes_in.shape, jnp.float32),
            pltpu.VMEM(slopes_in.shape, jnp.float32),
            pltpu.SemaphoreType.DMA((2, CHUNKS)),
        ],
        compiler_params=pltpu.CompilerParams(vmem_limit_bytes=16 * 2**20),
        name="momentum",
    )(*hbm)


def weights_kernel(weights, back, new_hbm, new, stored):
    chunks = stored.shape[0]
    per = new.shape[0] // chunks
    stores = []
    for c in range(chunks):

        def some(i, carry):
            part = pl.ds(c * per + i * BLOCK, BLOCK)
            new[part] = weights[part] - back[part]
            return carry

        lax.fori_loop(0, per // BLOCK, some, 0)
        part = pl.ds(c * per, per)
        stores.append(pltpu.make_async_copy(new.at[part], new_hbm.at[part], stored.at[c]))
        stores[-1].start()
    for copy in stores:
        copy.wait()


def weights_of(weights_in, back):
    return pl.pallas_call(
        weights_kernel,
        out_shape=jax.ShapeDtypeStruct(weights_in.shape, weights_in.dtype),
        in_specs=[pl.BlockSpec(memory_space=pltpu.VMEM)] * 2,
        out_specs=pl.BlockSpec(memory_space=pltpu.HBM),
        scratch_shapes=[
            pltpu.VMEM(weights_in.shape, jnp.float32),
            pltpu.SemaphoreType.DMA((CHUNKS,)),
        ],
        compiler_params=pltpu.CompilerParams(vmem_limit_bytes=16 * 2**20),
        name="new_weights",
    )(weights_in, back)


def body(slopes_in, moments_in, weights_in):
    momentum = momentum_of(slopes_in, moments_in)
    groups = lax.axis_size("fsdp")
    cuts = lax.axis_size("tp")
    mats, rows, cols = momentum.shape
    own = mats // (groups * cuts)
    moved = lax.all_to_all(
        momentum.reshape(groups * cuts, own, rows, cols), ("fsdp", "tp"), 0, 0, tiled=True
    )
    back, new_momentum = steps_of(moved.reshape(groups, cuts, own, rows, cols), momentum)
    back = lax.all_to_all(
        back.reshape(groups * cuts, own, rows, cols), ("fsdp", "tp"), 0, 0, tiled=True
    )
    new_weights = weights_of(weights_in, back.reshape(mats, rows, cols))
    return (new_weights, new_momentum)


def solution(mesh):
    placed = P("job", "fsdp", "tp")
    return jax.shard_map(
        body, mesh=mesh, in_specs=(placed,) * 3, out_specs=(placed,) * 2, check_vma=False
    )
```
